32 devices in a mesh: shard: 8 (over z, y), model: 4 (over x, core).
Axes of the slice: x: 2, y: 2, z: 4, core: 2. Of those that a mesh axis runs over, the one named last changes fastest.
Arguments:
- one_gate: float32 [2048, 8192], P('shard', 'model'), may hold values from -0.1875 to 0.1875
- other_gate: float32 [2048, 8192], P('shard', 'model'), may hold values from -0.125 to 0.125
- one_up: float32 [2048, 8192], P('shard', 'model'), may hold values from -0.1875 to 0.1875
- other_up: float32 [2048, 8192], P('shard', 'model'), may hold values from -0.125 to 0.125
- mix_share: float32 [2048], P('shard'), may hold values from 0.2 to 0.8
- norm_train: float32 [2048], P(('shard', 'model')), may hold values from 0.25 to 1.75
- norm_step: float32 [2048], P(('shard', 'model')), may hold values from -0.3 to 0.3
Outputs:
- final_gate: bfloat16 [2048, 8192], P(None, 'model')
- final_up: bfloat16 [2048, 8192], P(None, 'model')
- column_gate: float32 [8192], P('model')
- column_up: float32 [8192], P('model')
- serve_norm: bfloat16 [2048], replicated
The draws below stay inside these ranges and needn't reach their ends.
All inputs are finite; a program needn't handle non-finite values. Where the reference program divides by a largest or mean magnitude, that divisor is 1e-20 or more.
Results may differ from the reference program's by a relative error of at most 0.001.
Values may be sent and summed in bfloat16 or wider, within the bound.
A program may use at most 128 MiB of HBM per device.

```python
import jax
import jax.numpy as jnp

D_MODEL = 2048
D_INNER = 8192


def spiked(entries, rng, source, target, blocks, factor):
    def block_of(position):
        return (jnp.arange(entries.shape[position]) // (entries.shape[position] // blocks)).reshape((-1,) + (1,) * (entries.ndim - 1 - position))

    first = jax.random.permutation(rng, blocks)[block_of(target)]
    far = (block_of(target) + blocks // 2) % blocks
    return jnp.where((block_of(source) == first) | (block_of(source) == far), factor * entries, entries)


def level_of(rng, extent, shards, smallest, top_value):
    gain = 1.0
    for axis_at, parts in shards:
        draws = jax.random.uniform(jax.random.fold_in(jax.random.fold_in(rng, 6), axis_at), (parts,), jnp.float32, smallest / len(shards), top_value / len(shards))
        gain = gain * jnp.repeat(jnp.exp(draws), extent[axis_at] // parts).reshape((-1,) + (1,) * (len(extent) - 1 - axis_at))
    return gain


def centred(own_key, shape, scale, reach, split=(), held_as=jnp.bfloat16):
    values = scale * jax.random.normal(own_key, shape, jnp.float32)
    if split:
        values = values * level_of(own_key, shape, split, -0.22, 0.18)
    return jnp.clip(values, -reach, reach).astype(held_as)


def bell_draw_with(own_key, shape, width, limit, shards, heavy, kind=jnp.bfloat16):
    values = width * jax.random.normal(own_key, shape, jnp.float32)
    if shards:
        values = values * level_of(own_key, shape, shards, -0.22, 0.18)
    return jnp.clip(spiked(values, jax.random.fold_in(own_key, 3), *heavy), -limit, limit).astype(kind)


def setup_inputs(seed: int = 0) -> dict:
    keys = jax.random.split(jax.random.key(seed), 8)
    one_gate = bell_draw_with(keys[0], (D_MODEL, D_INNER), D_MODEL ** -0.5, 0.1875, ((0, 8), (1, 4)), (0, 1, 8, 2.0), jnp.float32)
    other_gate = centred(keys[1], (D_MODEL, D_INNER), D_MODEL ** -0.5, 0.125, ((0, 8), (1, 4)), jnp.float32)
    one_up = bell_draw_with(keys[2], (D_MODEL, D_INNER), D_MODEL ** -0.5, 0.1875, ((0, 8), (1, 4)), (0, 1, 8, 2.0), jnp.float32)
    other_up = centred(keys[3], (D_MODEL, D_INNER), D_MODEL ** -0.5, 0.125, ((0, 8), (1, 4)), jnp.float32)
    mix_share = jnp.clip(0.2 + 0.6 * jax.random.uniform(keys[4], (D_MODEL,), jnp.float32) ** level_of(keys[4], (D_MODEL,), ((0, 8),), -0.2, 0.2), 0.2, 0.8)
    norm_train = jnp.clip(1.0 + 0.15 * jax.random.normal(keys[5], (D_MODEL,), jnp.float32), 0.25, 1.75)
    norm_step = jnp.clip(jax.random.uniform(keys[6], (D_MODEL,), jnp.float32, -0.3, 0.3) * level_of(keys[6], (D_MODEL,), ((0, 32),), -0.4, 0.0), -0.3, 0.3)
    return {"one_gate": one_gate, "other_gate": other_gate, "one_up": one_up, "other_up": other_up, "mix_share": mix_share, "norm_train": norm_train, "norm_step": norm_step}


def reference(one_gate, other_gate, one_up, other_up, mix_share, norm_train, norm_step):
    result_gate = mix_share[:, None] * one_gate + (1.0 - mix_share[:, None]) * other_gate
    result_up = mix_share[:, None] * one_up + (1.0 - mix_share[:, None]) * other_up
    column_gate = jnp.max(jnp.abs(result_gate), axis=0)
    final_gate = (result_gate / column_gate).astype(jnp.bfloat16)
    column_up = jnp.max(jnp.abs(result_up), axis=0)
    final_up = (result_up / column_up).astype(jnp.bfloat16)
    serve_norm = (norm_train + norm_step).astype(jnp.bfloat16)
    return final_gate, final_up, column_gate, column_up, serve_norm
```

```python
import functools

import jax
import jax.numpy as jnp
from jax import lax
from jax.experimental import pallas as pl
from jax.experimental.pallas import tpu as pltpu
from jax.sharding import PartitionSpec as P

MESH = pl.DeviceIdType.MESH
LANES = 128


def position_of(index, n):
    return jnp.where(index % 2 == 0, index // 2, n - 1 - index // 2)


def index_at(position, n):
    return jnp.where(position < n // 2, 2 * position, 2 * (n - 1 - position) + 1)


def kernel(
    n, k, parts,
    one_gate, other_gate, one_up, other_up, mix, norm_train, norm_step,
    final_gate, final_up, column_gate, column_up, serve_norm,
    held_one, held_other, share, maxima_gate, maxima_up, gains,
    load_sem, max_send, max_recv, norm_send, norm_recv, ring_send, ring_recv,
):
    rows, cols = one_gate.shape
    piece = norm_train.shape[1]
    part = rows // parts
    me, col = lax.axis_index("shard"), lax.axis_index("model")
    at = position_of(me, n)

    ones, others = (one_gate, one_up), (other_gate, other_up)
    finals, columns, maxima = (final_gate, final_up), (column_gate, column_up), (maxima_gate, maxima_up)

    loads = {}
    for w in range(2):
        for c in range(parts):
            span = pl.ds(c * part, part)
            pair = (
                pltpu.make_async_copy(ones[w].at[span], held_one.at[w, span], load_sem.at[w, c, 0]),
                pltpu.make_async_copy(others[w].at[span], held_other.at[w, span], load_sem.at[w, c, 1]),
            )
            for copy in pair:
                copy.start()
            loads[w, c] = pair

    barrier = pltpu.get_barrier_semaphore()
    for d in range(1, n):
        pl.semaphore_signal(barrier, inc=1, device_id=((me + d) % n, col), device_id_type=MESH)
    for d in range(1, k):
        pl.semaphore_signal(barrier, inc=1, device_id=(me, (col + d) % k), device_id_type=MESH)

    share[...] = jnp.broadcast_to(mix[...], (LANES, rows)).T

    maxima_up[0, :, cols:cols + piece] = norm_train[...] + norm_step[...]

    def mixed(w):
        top = jnp.zeros((8, cols), jnp.float32)
        for c in range(parts):
            for copy in loads[w, c]:
                copy.wait()

            def step(g, top):
                span = pl.ds(pl.multiple_of(c * part + g * 8, 8), 8)
                m = share[span, 0:1]
                result = m * held_one[w, span, :] + (1.0 - m) * held_other[w, span, :]
                held_one[w, span, :] = result
                return jnp.maximum(top, jnp.abs(result))

            top = lax.fori_loop(0, part // 8, step, top, unroll=2)
        maxima[w][0, :, 0:cols] = jnp.max(top, axis=0, keepdims=True)

    def tell(w):
        copies = []
        for d in range(1, n):
            copy = pltpu.make_async_remote_copy(
                src_ref=maxima[w].at[0], dst_ref=maxima[w].at[d],
                send_sem=max_send.at[w, d], recv_sem=max_recv.at[w, d],
                device_id=((me + d) % n, col), device_id_type=MESH,
            )
            copy.start()
            copies.append(copy)
        return copies

    def ring(way, hop, w, c):
        origin = index_at((at + (n - hop if way == 0 else hop)) % n, n)
        span = pl.ds(pl.multiple_of(origin * rows + c * part, part), part)
        to = index_at((at + (1 if way == 0 else n - 1)) % n, n)
        return pltpu.make_async_remote_copy(
            src_ref=finals[w].at[span], dst_ref=finals[w].at[span],
            send_sem=ring_send.at[way, hop, w, c], recv_sem=ring_recv.at[way, hop, w, c],
            device_id=(to, col), device_id_type=MESH,
        )

    def scaled(w, c, inverse):
        def step(g, _):
            start = pl.multiple_of(c * part + g * 16, 16)
            to = pl.multiple_of(me * rows + c * part + g * 16, 16)
            finals[w][pl.ds(to, 16), :] = (held_one[w, pl.ds(start, 16), :] * inverse).astype(jnp.bfloat16)
            return 0

        lax.fori_loop(0, part // 16, step, 0)

    mixed(0)
    pl.semaphore_wait(barrier, n - 1 + k - 1)
    told = [tell(0)]
    mixed(1)
    told.append(tell(1))

    sent, norms = {}, []
    for w in range(2):
        for copy in told[w]:
            copy.wait_recv()
        column = jnp.max(maxima[w][:, :, 0:cols], axis=0)
        columns[w][...] = column
        inverse = 1.0 / column
        for c in range(parts):
            scaled(w, c, inverse)
            for way in range(2):
                sent[way, 0, w, c] = ring(way, 0, w, c)
                sent[way, 0, w, c].start()

    for d in range(n):
        gains[0, pl.ds((me + (n - d)) % n, 1), :] = maxima_up[d, :, cols:cols + LANES]
    for d in range(1, k):
        copy = pltpu.make_async_remote_copy(
            src_ref=gains.at[0], dst_ref=gains.at[d],
            send_sem=norm_send.at[d], recv_sem=norm_recv.at[d],
            device_id=(me, (col + d) % k), device_id_type=MESH,
        )
        copy.start()
        norms.append(copy)
    for copy in norms:
        copy.wait_recv()
    serve_norm[...] = jnp.concatenate(
        [gains[(col + (k - j)) % k][:, 0:piece] for j in range(k)], axis=1
    ).astype(jnp.bfloat16)

    for hop in range(1, n // 2 + 1):
        for w in range(2):
            for c in range(parts):
                for way in range(2):
                    if (way, hop - 1, w, c) not in sent:
                        continue
                    sent[way, hop - 1, w, c].wait_recv()
                    if hop < n // 2 - 1 or (hop == n // 2 - 1 and way == w):
                        sent[way, hop, w, c] = ring(way, hop, w, c)
                        sent[way, hop, w, c].start()

    for copy in sent.values():
        copy.wait_send()
    for copy in told[0] + told[1] + norms:
        copy.wait_send()


def solution(mesh):
    n, k = mesh.shape["shard"], mesh.shape["model"]

    def local(one_gate, other_gate, one_up, other_up, mix_share, norm_train, norm_step):
        rows, cols = one_gate.shape
        piece = norm_train.shape[0]
        parts = 4 if n <= 8 else 1
        whole = jax.ShapeDtypeStruct if n > 8 else pltpu.VMEM
        hbm, vmem = pl.BlockSpec(memory_space=pltpu.HBM), pl.BlockSpec(memory_space=pltpu.VMEM)
        final_gate, final_up, column_gate, column_up, serve_norm = pl.pallas_call(
            functools.partial(kernel, n, k, parts),
            out_shape=[
                whole((n * rows, cols), jnp.bfloat16),
                whole((n * rows, cols), jnp.bfloat16),
                jax.ShapeDtypeStruct((1, cols), jnp.float32),
                jax.ShapeDtypeStruct((1, cols), jnp.float32),
                jax.ShapeDtypeStruct((n, k * piece), jnp.bfloat16),
            ],
            in_specs=[hbm] * 4 + [vmem] * 3,
            out_specs=[vmem] * 5,
            scratch_shapes=[
                pltpu.VMEM((2, rows, cols), jnp.float32),
                pltpu.VMEM((2, rows, cols), jnp.float32),
                pltpu.VMEM((rows, LANES), jnp.float32),
                pltpu.VMEM((n, 1, cols), jnp.float32),
                pltpu.VMEM((n, 1, cols + LANES), jnp.float32),
                pltpu.VMEM((k, n, LANES), jnp.float32),
                pltpu.SemaphoreType.DMA((2, parts, 2)),
                pltpu.SemaphoreType.DMA((2, n)),
                pltpu.SemaphoreType.DMA((2, n)),
                pltpu.SemaphoreType.DMA((k,)),
                pltpu.SemaphoreType.DMA((k,)),
                pltpu.SemaphoreType.DMA((2, n // 2, 2, parts)),
                pltpu.SemaphoreType.DMA((2, n // 2, 2, parts)),
            ],
            compiler_params=pltpu.CompilerParams(
                collective_id=0, has_side_effects=True, vmem_limit_bytes=46 * 2**20
            ),
        )(
            one_gate, other_gate, one_up, other_up,
            mix_share.reshape(1, rows), norm_train.reshape(1, piece), norm_step.reshape(1, piece),
        )
        return (
            final_gate, final_up, column_gate.reshape(cols), column_up.reshape(cols),
            serve_norm.reshape(n * k * piece),
        )

    return jax.shard_map(
        local,
        mesh=mesh,
        in_specs=(
            P("shard", "model"), P("shard", "model"), P("shard", "model"), P("shard", "model"),
            P("shard"), P(("shard", "model")), P(("shard", "model")),
        ),
        out_specs=(P(None, "model"), P(None, "model"), P("model"), P("model"), P()),
        check_vma=False,
    )
```

```python
import functools

import jax
import jax.numpy as jnp
from jax import lax
from jax.experimental import pallas as pl
from jax.experimental.pallas import tpu as pltpu
from jax.sharding import PartitionSpec as P

MESH = pl.DeviceIdType.MESH
LANES = 128


def position_of(index, n):
    return jnp.where(index % 2 == 0, index // 2, n - 1 - index // 2)


def index_at(position, n):
    return jnp.where(position < n // 2, 2 * position, 2 * (n - 1 - position) + 1)


def kernel(
    n, k, parts,
    one_gate, other_gate, one_up, other_up, mix, norm_train, norm_step,
    final_gate, final_up, column_gate, column_up, serve_norm,
    held_one, held_other, share, maxima, gains, gain_rows,
    load_sem, max_send, max_recv, norm_send, norm_recv, ring_send, ring_recv,
):
    rows, cols = one_gate.shape
    piece = norm_train.shape[1]
    part = cols // parts
    me, col = lax.axis_index("shard"), lax.axis_index("model")
    at = position_of(me, n)

    ones, others = (one_gate, one_up), (other_gate, other_up)
    finals, columns = (final_gate, final_up), (column_gate, column_up)

    loads = {}
    for w in range(2):
        for c in range(parts):
            span = pl.ds(c * part, part)
            pair = (
                pltpu.make_async_copy(ones[w].at[:, span], held_one.at[w, :, span], load_sem.at[w, c, 0]),
                pltpu.make_async_copy(others[w].at[:, span], held_other.at[w, :, span], load_sem.at[w, c, 1]),
            )
            for copy in pair:
                copy.start()
            loads[w, c] = pair

    barrier = pltpu.get_barrier_semaphore()
    for d in range(1, n):
        pl.semaphore_signal(barrier, inc=1, device_id=((me + d) % n, col), device_id_type=MESH)
    for d in range(1, k):
        pl.semaphore_signal(barrier, inc=1, device_id=(me, (col + d) % k), device_id_type=MESH)

    share[...] = jnp.broadcast_to(mix[...], (LANES, rows)).T

    maxima[1, parts - 1, 0, :, part:part + piece] = norm_train[...] + norm_step[...]

    def mixed(w, c):
        for copy in loads[w, c]:
            copy.wait()
        span = pl.ds(c * part, part)

        def step(g, top):
            lines = pl.ds(pl.multiple_of(g * 8, 8), 8)
            m = share[lines, 0:1]
            result = m * held_one[w, lines, span] + (1.0 - m) * held_other[w, lines, span]
            held_one[w, lines, span] = result
            return jnp.maximum(top, jnp.abs(result))

        top = lax.fori_loop(0, rows // 8, step, jnp.zeros((8, part), jnp.float32), unroll=4)
        maxima[w, c, 0, :, 0:part] = jnp.max(top, axis=0, keepdims=True)

    def tell(w, c):
        width = part + LANES if (w, c) == (1, parts - 1) else part
        copies = []
        for d in range(1, n):
            copy = pltpu.make_async_remote_copy(
                src_ref=maxima.at[w, c, 0, :, pl.ds(0, width)], dst_ref=maxima.at[w, c, d, :, pl.ds(0, width)],
                send_sem=max_send.at[w, c, d], recv_sem=max_recv.at[w, c, d],
                device_id=((me + d) % n, col), device_id_type=MESH,
            )
            copy.start()
            copies.append(copy)
        return copies

    def ring(way, hop, w, c):
        origin = index_at((at + (n - hop if way == 0 else hop)) % n, n)
        lines, span = pl.ds(pl.multiple_of(origin * rows, rows), rows), pl.ds(c * part, part)
        to = index_at((at + (1 if way == 0 else n - 1)) % n, n)
        return pltpu.make_async_remote_copy(
            src_ref=finals[w].at[lines, span], dst_ref=finals[w].at[lines, span],
            send_sem=ring_send.at[way, hop, w, c], recv_sem=ring_recv.at[way, hop, w, c],
            device_id=(to, col), device_id_type=MESH,
        )

    def scaled(w, c, inverse):
        span = pl.ds(c * part, part)

        def step(g, _):
            start = pl.multiple_of(g * 16, 16)
            to = pl.multiple_of(me * rows + g * 16, 16)
            finals[w][pl.ds(to, 16), span] = (held_one[w, pl.ds(start, 16), span] * inverse).astype(jnp.bfloat16)
            return 0

        lax.fori_loop(0, rows // 16, step, 0, unroll=2)

    units = [(w, c) for w in range(2) for c in range(parts)]
    told = {}
    for w, c in units:
        mixed(w, c)
        if (w, c) == units[0]:
            pl.semaphore_wait(barrier, n - 1 + k - 1)
        told[w, c] = tell(w, c)

    sent, norms = {}, []
    for w, c in units:
        for copy in told[w, c]:
            copy.wait_recv()
        column = jnp.max(maxima[w, c, :, :, 0:part], axis=0)
        columns[w][:, pl.ds(c * part, part)] = column
        scaled(w, c, 1.0 / column)
        for way in range(2):
            sent[way, 0, w, c] = ring(way, 0, w, c)
            sent[way, 0, w, c].start()

    for d in range(n):
        gains[0, pl.ds((me + (n - d)) % n, 1), :] = maxima[1, parts - 1, d, :, part:part + LANES]
    for d in range(1, k):
        copy = pltpu.make_async_remote_copy(
            src_ref=gains.at[0], dst_ref=gains.at[d],
            send_sem=norm_send.at[d], recv_sem=norm_recv.at[d],
            device_id=(me, (col + d) % k), device_id_type=MESH,
        )
        copy.start()
        norms.append(copy)
    for copy in norms:
        copy.wait_recv()
    gain = jnp.concatenate([gains[(col + (k - j)) % k][:, 0:piece] for j in range(k)], axis=1)
    if serve_norm.shape[1] == gain.shape[1]:
        serve_norm[...] = gain.astype(jnp.bfloat16)
    else:
        each = k * piece // LANES
        for i in range(n * each):
            at_lane = i % each * LANES
            gain_rows[i:i + 1, :] = gain[i // each:i // each + 1, at_lane:at_lane + LANES]
        serve_norm[...] = gain_rows[...].astype(jnp.bfloat16)

    for hop in range(1, n // 2 + 1):
        for w in range(2):
            for c in range(parts):
                for way in range(2):
                    if (way, hop - 1, w, c) not in sent:
                        continue
                    sent[way, hop - 1, w, c].wait_recv()
                    if hop < n // 2 - 1 or (hop == n // 2 - 1 and way == w):
                        sent[way, hop, w, c] = ring(way, hop, w, c)
                        sent[way, hop, w, c].start()

    for copy in sent.values():
        copy.wait_send()
    for copy in sum(told.values(), norms):
        copy.wait_send()


def writer(*refs):
    (sem,), count = refs[-1:], (len(refs) - 1) // 2
    copies = []
    for source, target in zip(refs[:count], refs[count:-1]):
        pieces = 4 if source.shape[0] > LANES else 1
        lines = source.shape[0] // pieces
        for p in range(pieces):
            span = pl.ds(p * lines, lines)
            copies.append(pltpu.make_async_copy(source.at[span], target.at[span], sem.at[len(copies)]))
    for copy in copies:
        copy.start()
    for copy in copies:
        copy.wait()


def solution(mesh):
    n, k = mesh.shape["shard"], mesh.shape["model"]

    def local(one_gate, other_gate, one_up, other_up, mix_share, norm_train, norm_step):
        rows, cols = one_gate.shape
        piece = norm_train.shape[0]
        parts = 2 if n <= 8 else 1
        near = n <= 8
        shaped = pltpu.VMEM if near else jax.ShapeDtypeStruct
        norm_shape = (n * k * piece // LANES, LANES) if k * piece % LANES == 0 else (n, k * piece)
        shapes = [
            ((n * rows, cols), jnp.bfloat16), ((n * rows, cols), jnp.bfloat16),
            ((1, cols), jnp.float32), ((1, cols), jnp.float32), (norm_shape, jnp.bfloat16),
        ]
        hbm, vmem = pl.BlockSpec(memory_space=pltpu.HBM), pl.BlockSpec(memory_space=pltpu.VMEM)
        results = pl.pallas_call(
            functools.partial(kernel, n, k, parts),
            out_shape=[shaped(*shape) for shape in shapes],
            in_specs=[hbm] * 4 + [vmem] * 3,
            out_specs=[vmem] * 5,
            scratch_shapes=[
                pltpu.VMEM((2, rows, cols), jnp.float32),
                pltpu.VMEM((2, rows, cols), jnp.float32),
                pltpu.VMEM((rows, LANES), jnp.float32),
                pltpu.VMEM((2, parts, n, 1, cols // parts + LANES), jnp.float32),
                pltpu.VMEM((k, n, LANES), jnp.float32),
                pltpu.VMEM((max(n * k * piece // LANES, 8), LANES), jnp.float32),
                pltpu.SemaphoreType.DMA((2, parts, 2)),
                pltpu.SemaphoreType.DMA((2, parts, n)),
                pltpu.SemaphoreType.DMA((2, parts, n)),
                pltpu.SemaphoreType.DMA((k,)),
                pltpu.SemaphoreType.DMA((k,)),
                pltpu.SemaphoreType.DMA((2, n // 2, 2, parts)),
                pltpu.SemaphoreType.DMA((2, n // 2, 2, parts)),
            ],
            compiler_params=pltpu.CompilerParams(
                collective_id=0, has_side_effects=True, vmem_limit_bytes=46 * 2**20
            ),
        )(
            one_gate, other_gate, one_up, other_up,
            mix_share.reshape(1, rows), norm_train.reshape(1, piece), norm_step.reshape(1, piece),
        )
        if near:
            results = pl.pallas_call(
                writer,
                out_shape=[jax.ShapeDtypeStruct(*shape) for shape in shapes],
                in_specs=[vmem] * 5,
                out_specs=[hbm] * 5,
                scratch_shapes=[pltpu.SemaphoreType.DMA((11,))],
                compiler_params=pltpu.CompilerParams(vmem_limit_bytes=2**20),
            )(*results)
        final_gate, final_up, column_gate, column_up, serve_norm = results
        return (
            final_gate, final_up, column_gate.reshape(cols), column_up.reshape(cols),
            serve_norm.reshape(n * k * piece),
        )

    return jax.shard_map(
        local,
        mesh=mesh,
        in_specs=(
            P("shard", "model"), P("shard", "model"), P("shard", "model"), P("shard", "model"),
            P("shard"), P(("shard", "model")), P(("shard", "model")),
        ),
        out_specs=(P(None, "model"), P(None, "model"), P("model"), P("model"), P()),
        check_vma=False,
    )
```
